32 devices in a mesh: gz: 8 (over z, x), col: 4 (over y, core).
Axes of the slice: x: 2, y: 2, z: 4, core: 2. Of those that a mesh axis runs over, the one named last changes fastest.
Arguments:
- features: bfloat16 [64, 16, 128, 128], P(None, 'gz'), may hold values from -6 to 6
- grad_out: bfloat16 [64, 16, 128, 128], P('col', 'gz'), may hold values from -6 to 6
- conv_weight: bfloat16 [64, 64, 27], P('col'), may hold values from -0.15625 to 0.15625
- spectral_weight: bfloat16 [64, 64, 16, 256], P(None, 'col', None, 'gz'), may hold values from -3 to 3
Outputs:
- layer_out: bfloat16 [64, 16, 128, 128], P('col', 'gz')
- grad_input: bfloat16 [64, 16, 128, 128], P('col', 'gz')
- grad_conv: float32 [64, 64, 27], P('col')
- grad_spectral: float32 [64, 64, 16, 256], P(None, 'col', None, 'gz')
The draws below stay inside these ranges and needn't reach their ends.
All inputs are finite; a program needn't handle non-finite values.
Results may differ from the reference program's by a relative error of at most 0.008.
Values may be sent and summed in bfloat16 or wider, within the bound.
A program may use at most 256 MiB of HBM per device.

```python
import math
from functools import partial
import jax
import jax.numpy as jnp
from jax import lax

WIDTH = 64
NX = 128
NY = 128
MODES = 16
NZ = 16


def block_levels(own_key, shape, cuts, low, largest):
    level = 1.0
    for position, shards_of in cuts:
        heights = jax.random.uniform(jax.random.fold_in(jax.random.fold_in(own_key, 6), position), (shards_of,), jnp.float32, low / len(cuts), largest / len(cuts))
        level = level * jnp.repeat(jnp.exp(heights), shape[position] // shards_of).reshape((-1,) + (1,) * (len(shape) - 1 - position))
    return level


def centred(key, extent, scale, bound, split=(), kind=jnp.bfloat16):
    result = scale * jax.random.normal(key, extent, jnp.float32)
    if split:
        result = result * block_levels(key, extent, split, -0.22, 0.18)
    return jnp.clip(result, -bound, bound).astype(kind)


def setup_inputs(seed: int = 0) -> dict:
    arg_keys = jax.random.split(jax.random.key(seed), 5)
    return {
        "features": centred(arg_keys[0], (WIDTH, NZ, NX, NY), 1.0, 6.0, ((1, 8),)),
        "grad_out": centred(arg_keys[1], (WIDTH, NZ, NX, NY), 1.0, 6.0, ((0, 4), (1, 8))),
        "conv_weight": centred(arg_keys[2], (WIDTH, WIDTH, 27), (27 * WIDTH) ** -0.5, 0.15625, ((0, 4),)),
        "spectral_weight": centred(arg_keys[3], (WIDTH, WIDTH, MODES, MODES * MODES), 0.5, 3.0, ((1, 4), (3, 8))),
    }


highest = lax.Precision.HIGHEST

def basis(length, mode_count):
    indices = jnp.arange(mode_count, dtype=jnp.int32)
    middle = mode_count // 2
    cosine_rows = indices <= middle
    frequency = jnp.where(cosine_rows, indices, indices - middle)
    positions = jnp.arange(length, dtype=jnp.int32)
    residue = frequency[:, None] * positions[None, :] % length
    radians = residue.astype(jnp.float32) * (2.0 * math.pi / length)
    tables = jnp.where(cosine_rows[:, None], jnp.cos(radians), jnp.sin(radians))
    return tables * math.sqrt(2.0 / length)

def activate(preact, cotangent):
    outcome, pullback = jax.vjp(partial(jax.nn.gelu, approximate=True), preact)
    return (outcome, pullback(cotangent)[0])

def shift_of(offset, direction):
    return (direction * (1 - offset // 9), direction * (1 - offset // 3 % 3), direction * (1 - offset % 3))

def reference(features, grad_out, conv_weight, spectral_weight):
    table_x = basis(NX, MODES)
    table_y = basis(NY, MODES)
    table_z = basis(NZ, MODES)
    cell_count = NZ * NX * NY

    def analyse(volume):
        along_y = jnp.dot(volume.reshape(WIDTH * NZ * NX, NY), table_y.astype(jnp.bfloat16).T, preferred_element_type=jnp.float32)
        along_y = along_y.reshape(WIDTH, NZ, NX, MODES)
        along_x = jnp.einsum('kx,czxl->czkl', table_x, along_y, precision=highest)
        along_z = jnp.einsum('jz,czkl->cjkl', table_z, along_x, precision=highest)
        return along_z.reshape(WIDTH, MODES, MODES * MODES)

    def synthesise(spectrum):
        blocks = spectrum.reshape(WIDTH, MODES, MODES, MODES)
        along_z = jnp.einsum('jz,cjkl->czkl', table_z, blocks, precision=highest)
        along_x = jnp.einsum('kx,czkl->czxl', table_x, along_z, precision=highest)
        return jnp.einsum('czxl,ly->czxy', along_x, table_y, precision=highest)
    conv_sum = jnp.zeros((WIDTH, cell_count), jnp.float32)
    for offset in range(27):
        moved = jnp.roll(features, shift_of(offset, 1), axis=(1, 2, 3)).reshape(WIDTH, cell_count)
        conv_sum = conv_sum + jnp.dot(conv_weight[:, :, offset], moved, preferred_element_type=jnp.float32)
    weights32 = spectral_weight.astype(jnp.float32)
    spectrum = analyse(features)
    mixed = jnp.einsum('iokm,ikm->okm', weights32, spectrum, precision=highest)
    preact = conv_sum.reshape(WIDTH, NZ, NX, NY) + synthesise(mixed)
    outcome, slope = activate(preact, grad_out.astype(jnp.float32))
    layer_out = outcome.astype(jnp.bfloat16)
    grad_pre = slope.astype(jnp.bfloat16)
    flat_grad = grad_pre.reshape(WIDTH, cell_count)
    back_conv = jnp.zeros((WIDTH, cell_count), jnp.float32)
    kernel_grads = []
    for offset in range(27):
        moved_grad = jnp.roll(grad_pre, shift_of(offset, -1), axis=(1, 2, 3)).reshape(WIDTH, cell_count)
        back_conv = back_conv + jnp.dot(conv_weight[:, :, offset].T, moved_grad, preferred_element_type=jnp.float32)
        moved = jnp.roll(features, shift_of(offset, 1), axis=(1, 2, 3)).reshape(WIDTH, cell_count)
        kernel_grads.append(lax.dot_general(flat_grad, moved, (((1,), (1,)), ((), ())), preferred_element_type=jnp.float32))
    scaling = 1.0 / math.sqrt(NX * NY * NZ)
    grad_conv = jnp.stack(kernel_grads, axis=2) * scaling
    grad_modes = analyse(grad_pre)
    back_modes = jnp.einsum('iokm,okm->ikm', weights32, grad_modes, precision=highest)
    grad_input = (back_conv.reshape(WIDTH, NZ, NX, NY) + synthesise(back_modes)).astype(jnp.bfloat16)
    grad_spectral = spectrum[:, None] * grad_modes[None]
    return (layer_out, grad_input, grad_conv, grad_spectral)
```

```python
from functools import partial
import math

import jax
import jax.numpy as jnp
import numpy as np
from jax import lax
from jax.experimental import pallas as pl
from jax.experimental.pallas import tpu as pltpu
from jax.sharding import PartitionSpec as P

highest = lax.Precision.HIGHEST
f32 = jnp.float32
bf16 = jnp.bfloat16


def basis(length, mode_count):
    indices = np.arange(mode_count)
    middle = mode_count // 2
    cosine_rows = indices <= middle
    frequency = np.where(cosine_rows, indices, indices - middle)
    residue = frequency[:, None] * np.arange(length)[None, :] % length
    radians = residue * (2.0 * math.pi / length)
    tables = np.where(cosine_rows[:, None], np.cos(radians), np.sin(radians))
    return (tables * math.sqrt(2.0 / length)).astype(np.float32)


def split_table(table):
    high = table.astype(bf16)
    return high, (table - high.astype(np.float32)).astype(bf16)


def neighbours(axis):
    count = lax.axis_size(axis)
    up = [(i, (i + 1) % count) for i in range(count)]
    down = [((i + 1) % count, i) for i in range(count)]
    return up, down


def params(*semantics):
    return pltpu.CompilerParams(
        dimension_semantics=semantics, vmem_limit_bytes=48 * 1024 * 1024
    )


def slab_modes(slab_of, count, ex2, eyt):
    modes = ex2.shape[0] // 2
    parts = []
    for s in range(count):
        both = jnp.dot(ex2, slab_of(s), preferred_element_type=f32)
        parts.append(both[:modes] + both[modes:])
    along_x = jnp.concatenate(parts, axis=0)
    high = along_x.astype(bf16)
    low = (along_x - high.astype(f32)).astype(bf16)
    return jnp.dot(high, eyt, preferred_element_type=f32) + jnp.dot(
        low, eyt, preferred_element_type=f32
    )


def analyse_kernel(v_ref, ex_ref, ey_ref, o_ref):
    count = v_ref.shape[0]
    ex2, eyt = ex_ref[...], ey_ref[...]
    out = slab_modes(lambda s: v_ref[s], count, ex2, eyt)
    o_ref[...] = out.reshape(o_ref.shape)


def analyse_slabs(volume, ex2, eyt):
    slabs, size_x, size_y = volume.shape
    modes = eyt.shape[1]
    block = 16
    return pl.pallas_call(
        analyse_kernel,
        grid=(slabs // block,),
        in_specs=[
            pl.BlockSpec((block, size_x, size_y), lambda g: (g, 0, 0)),
            pl.BlockSpec(ex2.shape, lambda g: (0, 0)),
            pl.BlockSpec(eyt.shape, lambda g: (0, 0)),
        ],
        out_specs=pl.BlockSpec((block, modes, modes), lambda g: (g, 0, 0)),
        out_shape=jax.ShapeDtypeStruct((slabs, modes, modes), f32),
        compiler_params=params("arbitrary"),
        name="analyse",
    )(volume, ex2, eyt)


def conv_kernel(rows, size_y, f_ref, w_ref, o_ref):
    start = pl.program_id(0) * rows * size_y
    total = None
    depth = f_ref.shape[0]
    span = rows * size_y
    for b in range(3):
        first = pl.multiple_of(start + b * size_y, size_y)
        part = jnp.dot(
            w_ref[:, b * depth : (b + 1) * depth],
            f_ref[:, pl.ds(first, span)],
            preferred_element_type=f32,
        )
        total = part if total is None else total + part
    count = total.shape[0] // 3
    flat = o_ref.reshape(count * rows, size_y)
    for r in range(rows):
        piece = total[:, r * size_y : (r + 1) * size_y]
        value = (
            pltpu.roll(piece[:count], 1, 1)
            + piece[count : 2 * count]
            + pltpu.roll(piece[2 * count :], size_y - 1, 1)
        )
        flat[pl.ds(r, count, stride=rows), :] = value


def forward_conv(framed, weights, size_x, size_y):
    count = weights.shape[0] // 3
    rows = 8
    return pl.pallas_call(
        partial(conv_kernel, rows, size_y),
        grid=(size_x // rows,),
        in_specs=[
            pl.BlockSpec(framed.shape, lambda g: (0, 0)),
            pl.BlockSpec(weights.shape, lambda g: (0, 0)),
        ],
        out_specs=pl.BlockSpec((count, rows, size_y), lambda g: (0, g, 0)),
        out_shape=jax.ShapeDtypeStruct((count, size_x, size_y), f32),
        compiler_params=params("arbitrary"),
        name="forward_conv",
    )(framed, weights)


def planar(spectrum, ext, ey):
    along_x = jnp.dot(ext, spectrum, precision=highest, preferred_element_type=f32)
    return jnp.dot(along_x, ey, precision=highest, preferred_element_type=f32)


def gelu_kernel(c_ref, lo_ref, hi_ref, s_ref, g_ref, ext_ref, ey_ref, ex2_ref, eyt_ref,
                out_ref, gp_ref, m_ref):
    plane = pl.program_id(0)
    last = pl.num_programs(0) - 1
    count = c_ref.shape[1]
    keep_lo = jnp.where(plane == 0, 1.0, 0.0).astype(f32)
    keep_hi = jnp.where(plane == last, 1.0, 0.0).astype(f32)
    ext, ey = ext_ref[...], ey_ref[...]
    k0 = math.sqrt(2.0 / math.pi)
    k1 = 0.044715
    for o in range(count):
        v = c_ref[0, o] + lo_ref[o].astype(f32) * keep_lo + hi_ref[o].astype(f32) * keep_hi
        v = v + planar(s_ref[0, o], ext, ey)
        v2 = v * v
        t = jnp.tanh(k0 * v * (1.0 + k1 * v2))
        half = 0.5 * (1.0 + t)
        out_ref[o, 0] = (v * half).astype(bf16)
        slope = half + (0.5 * k0) * v * (1.0 - t * t) * (1.0 + (3.0 * k1) * v2)
        gp_ref[o, 0] = (g_ref[o, 0].astype(f32) * slope).astype(bf16)
    modes = slab_modes(lambda o: gp_ref[o, 0], count, ex2_ref[...], eyt_ref[...])
    m_ref[...] = modes.reshape(m_ref.shape)


def gelu_stage(conv, low, high, slabs, grad_out, tables):
    ext, ey, ex2, eyt = tables
    share, planes, size_x, size_y = grad_out.shape
    modes = ey.shape[0]
    block = 8
    field = pl.BlockSpec((block, 1, size_x, size_y), lambda z, g: (g, z, 0, 0))
    rim = pl.BlockSpec((block, size_x, size_y), lambda z, g: (g, 0, 0))
    whole = lambda t: pl.BlockSpec(t.shape, lambda z, g: (0, 0))
    return pl.pallas_call(
        gelu_kernel,
        grid=(planes, share // block),
        in_specs=[
            pl.BlockSpec((1, block, size_x, size_y), lambda z, g: (z + 1, g, 0, 0)),
            rim,
            rim,
            pl.BlockSpec((1, block, modes, modes), lambda z, g: (z, g, 0, 0)),
            field,
            whole(ext),
            whole(ey),
            whole(ex2),
            whole(eyt),
        ],
        out_specs=[
            field,
            field,
            pl.BlockSpec((1, block, modes, modes), lambda z, g: (z, g, 0, 0)),
        ],
        out_shape=[
            jax.ShapeDtypeStruct(grad_out.shape, bf16),
            jax.ShapeDtypeStruct(grad_out.shape, bf16),
            jax.ShapeDtypeStruct((planes, share, modes, modes), f32),
        ],
        compiler_params=params("arbitrary", "arbitrary"),
        name="gelu_stage",
    )(conv, low, high, slabs, grad_out, ext, ey, ex2, eyt)


def back_kernel(rows, size_y, g_ref, f_ref, w_ref, c_ref, acc_ref, roll_ref):
    step = pl.program_id(0)
    height = g_ref.shape[0]
    span = rows * size_y

    @pl.when(step == 0)
    def _():
        acc_ref[...] = jnp.zeros_like(acc_ref)

        def shift(r, carry):
            lanes = pl.ds(pl.multiple_of(r * size_y, size_y), size_y)
            block = g_ref[:, lanes]
            wide = block.astype(f32)
            roll_ref[:height, lanes] = pltpu.roll(wide, size_y - 1, 1).astype(bf16)
            roll_ref[height : 2 * height, lanes] = block
            roll_ref[2 * height :, lanes] = pltpu.roll(wide, 1, 1).astype(bf16)
            return carry

        lax.fori_loop(0, g_ref.shape[1] // size_y, shift, 0)

    start = step * span
    shifted = []
    for b in range(3):
        first = pl.multiple_of(start + (2 - b) * size_y, size_y)
        shifted.append(roll_ref[:, pl.ds(first, span)])
    stacked = jnp.concatenate(shifted, axis=0)
    c_ref[...] = jnp.dot(w_ref[...], stacked, preferred_element_type=f32).astype(bf16)
    acc_ref[...] += lax.dot_general(
        stacked, f_ref[...], (((1,), (1,)), ((), ())), preferred_element_type=f32
    )


def backward_convs(grad_framed, framed, weights, size_x, size_y):
    height = grad_framed.shape[0]
    depth = framed.shape[0]
    rows = 8
    span = rows * size_y
    return pl.pallas_call(
        partial(back_kernel, rows, size_y),
        grid=(size_x // rows,),
        in_specs=[
            pl.BlockSpec(grad_framed.shape, lambda g: (0, 0)),
            pl.BlockSpec((depth, span), lambda g: (0, g)),
            pl.BlockSpec(weights.shape, lambda g: (0, 0)),
        ],
        out_specs=[
            pl.BlockSpec((depth, span), lambda g: (0, g)),
            pl.BlockSpec((9 * height, depth), lambda g: (0, 0)),
        ],
        out_shape=[
            jax.ShapeDtypeStruct((depth, size_x * size_y), bf16),
            jax.ShapeDtypeStruct((9 * height, depth), f32),
        ],
        scratch_shapes=[pltpu.VMEM((3 * height, grad_framed.shape[1]), bf16)],
        compiler_params=params("arbitrary"),
        name="backward_convs",
    )(grad_framed, framed, weights)


def final_kernel(a_ref, b_ref, s_ref, ext_ref, ey_ref, o_ref):
    ext, ey = ext_ref[...], ey_ref[...]
    for i in range(a_ref.shape[0]):
        total = a_ref[i].astype(f32) + b_ref[i].astype(f32) + planar(s_ref[i], ext, ey)
        o_ref[i] = total.astype(bf16)


def final_stage(own, other, slabs, tables):
    ext, ey = tables[:2]
    count, size_x, size_y = own.shape
    modes = ey.shape[0]
    block = 8
    field = pl.BlockSpec((block, size_x, size_y), lambda g: (g, 0, 0))
    return pl.pallas_call(
        final_kernel,
        grid=(count // block,),
        in_specs=[
            field,
            field,
            pl.BlockSpec((block, modes, modes), lambda g: (g, 0, 0)),
            pl.BlockSpec(ext.shape, lambda g: (0, 0)),
            pl.BlockSpec(ey.shape, lambda g: (0, 0)),
        ],
        out_specs=field,
        out_shape=jax.ShapeDtypeStruct(own.shape, bf16),
        compiler_params=params("arbitrary"),
        name="final_stage",
    )(own, other, slabs, ext, ey)


def to_modes(planes, table_z):
    gathered = lax.all_to_all(planes, "gz", split_axis=2, concat_axis=1, tiled=True)
    return jnp.einsum("jz,czm->cjm", table_z, gathered, precision=highest)


def to_slabs(spectrum, table_z):
    columns = jnp.einsum("jz,cjm->czm", table_z, spectrum, precision=highest)
    return lax.all_to_all(columns, "gz", split_axis=1, concat_axis=2, tiled=True)


def halve(block, bit):
    count = lax.axis_size("col")
    side = (lax.axis_index("col") // bit) % 2
    pairs = [(i, i ^ bit) for i in range(count)]
    mine = lax.dynamic_index_in_dim(block, side, 0, keepdims=False)
    other = lax.dynamic_index_in_dim(block, 1 - side, 0, keepdims=False)
    return mine, lax.ppermute(other, "col", pairs)


def frame(flat, size_y):
    return jnp.concatenate([flat[:, -size_y:], flat, flat[:, :size_y]], axis=1)


def local(features, grad_out, conv_weight, spectral_weight):
    channels, planes, size_x, size_y = features.shape
    share = conv_weight.shape[0]
    modes = spectral_weight.shape[2]
    groups = lax.axis_size("gz")
    parts = lax.axis_size("col")
    table_x = basis(size_x, modes)
    table_y = basis(size_y, modes)
    table_z = basis(planes * groups, modes)
    ex2 = np.concatenate(split_table(table_x), axis=0)
    eyt = np.ascontiguousarray(table_y.astype(bf16).T)
    tables = tuple(
        jnp.asarray(t) for t in (np.ascontiguousarray(table_x.T), table_y, ex2, eyt)
    )
    table_z = jnp.asarray(table_z)
    up, down = neighbours("gz")

    pick = np.zeros((3, planes, planes + 2), np.float32)
    for z in range(planes):
        for a in range(3):
            pick[a, z, z - a + 2] = 1.0
    kernel = conv_weight.reshape(share, channels, 3, 3, 3)
    spread = jnp.einsum(
        "oiabc,azp->oizpbc", kernel, jnp.asarray(pick, bf16), preferred_element_type=bf16
    )
    w_forward = jnp.transpose(spread, (5, 3, 0, 4, 1, 2)).reshape(
        3 * (planes + 2) * share, 3 * channels * planes
    )
    w_back = jnp.transpose(spread, (1, 2, 4, 5, 0, 3)).reshape(
        channels * planes, 9 * share * (planes + 2)
    )

    first_channel = lax.axis_index("col") * share
    own = lax.dynamic_slice_in_dim(features, first_channel, share, 0)
    planar_modes = analyse_slabs(own.reshape(share * planes, size_x, size_y), *tables[2:])
    spectrum = to_modes(planar_modes.reshape(share, planes, modes * modes), table_z)
    spectrum_all = lax.all_gather(spectrum, "col", axis=0, tiled=True)

    framed = frame(features.reshape(channels * planes, size_x * size_y), size_y)
    conv = forward_conv(framed, w_forward, size_x, size_y)
    conv = conv.reshape(planes + 2, share, size_x, size_y)
    low = lax.ppermute(conv[planes + 1].astype(bf16), "gz", up)
    high = lax.ppermute(conv[0].astype(bf16), "gz", down)

    weights32 = spectral_weight.astype(f32)
    mixed = jnp.sum(weights32 * spectrum_all[:, None], axis=0)
    slabs = to_slabs(mixed, table_z)
    slabs = jnp.transpose(slabs.reshape(share, planes, modes, modes), (1, 0, 2, 3))
    layer_out, grad_pre, grad_planar = gelu_stage(conv, low, high, slabs, grad_out, tables)

    before = lax.ppermute(grad_pre[:, planes - 1 :], "gz", up)
    after = lax.ppermute(grad_pre[:, :1], "gz", down)
    grad_planar = jnp.transpose(grad_planar, (1, 0, 2, 3)).reshape(share, planes, modes * modes)
    grad_modes = to_modes(grad_planar, table_z)

    rimmed = jnp.concatenate([before, grad_pre, after], axis=1)
    grad_framed = frame(rimmed.reshape(share * (planes + 2), size_x * size_y), size_y)
    contributions, products = backward_convs(
        grad_framed, framed[:, size_y:-size_y], w_back, size_x, size_y
    )
    block = contributions.reshape(parts, share * planes, size_x * size_y)
    bit = 1
    received = None
    while bit < parts:
        if received is not None:
            block = (block.astype(f32) + received.astype(f32)).astype(bf16)
        paired = block.reshape(block.shape[0] // 2, 2, *block.shape[1:])
        block, received = halve(jnp.swapaxes(paired, 0, 1), bit)
        bit *= 2
    shape = (share * planes, size_x, size_y)
    block, received = block.reshape(shape), received.reshape(shape)

    products = products.reshape(3, 3, share, planes + 2, channels, planes)
    taps = [
        sum(products[:, :, :, z - a + 2, :, z] for z in range(planes)) for a in range(3)
    ]
    local_grad = jnp.stack(taps, axis=0)
    scaling = 1.0 / math.sqrt(size_x * size_y * planes * groups)
    grad_conv = lax.psum(local_grad.reshape(27 * share, channels), "gz") * scaling
    grad_conv = jnp.transpose(grad_conv.reshape(27, share, channels), (1, 2, 0))

    back_terms = jnp.sum(weights32 * grad_modes[None], axis=1)
    back_modes = lax.psum_scatter(
        back_terms.astype(bf16), "col", scatter_dimension=0, tiled=True
    ).astype(f32)
    back_slabs = to_slabs(back_modes, table_z).reshape(share * planes, modes, modes)
    grad_input = final_stage(block, received, back_slabs, tables)
    grad_input = grad_input.reshape(share, planes, size_x, size_y)
    grad_spectral = spectrum_all[:, None] * grad_modes[None]
    return (layer_out, grad_input, grad_conv, grad_spectral)


def solution(mesh):
    return jax.shard_map(
        local,
        mesh=mesh,
        in_specs=(
            P(None, "gz", None, None),
            P("col", "gz", None, None),
            P("col", None, None),
            P(None, "col", None, "gz"),
        ),
        out_specs=(
            P("col", "gz", None, None),
            P("col", "gz", None, None),
            P("col", None, None),
            P(None, "col", None, "gz"),
        ),
        check_vma=False,
    )
```

```python
from functools import partial
import math

import jax
import jax.numpy as jnp
import numpy as np
from jax import lax
from jax.experimental import pallas as pl
from jax.experimental.pallas import tpu as pltpu
from jax.sharding import PartitionSpec as P

highest = lax.Precision.HIGHEST
f32 = jnp.float32
bf16 = jnp.bfloat16


def basis(length, mode_count):
    indices = np.arange(mode_count)
    middle = mode_count // 2
    cosine_rows = indices <= middle
    frequency = np.where(cosine_rows, indices, indices - middle)
    residue = frequency[:, None] * np.arange(length)[None, :] % length
    radians = residue * (2.0 * math.pi / length)
    tables = np.where(cosine_rows[:, None], np.cos(radians), np.sin(radians))
    return (tables * math.sqrt(2.0 / length)).astype(np.float32)


def split_table(table):
    high = table.astype(bf16)
    return high, (table - high.astype(np.float32)).astype(bf16)


def neighbours(axis):
    count = lax.axis_size(axis)
    up = [(i, (i + 1) % count) for i in range(count)]
    down = [((i + 1) % count, i) for i in range(count)]
    return up, down


def params(*semantics):
    return pltpu.CompilerParams(
        dimension_semantics=semantics, vmem_limit_bytes=48 * 1024 * 1024
    )


def slab_modes(slab_of, count, ex2, eyt):
    modes = ex2.shape[0] // 2
    parts = []
    for s in range(count):
        both = jnp.dot(ex2, slab_of(s), preferred_element_type=f32)
        parts.append(both[:modes] + both[modes:])
    along_x = jnp.concatenate(parts, axis=0)
    high = along_x.astype(bf16)
    low = (along_x - high.astype(f32)).astype(bf16)
    return jnp.dot(high, eyt, preferred_element_type=f32) + jnp.dot(
        low, eyt, preferred_element_type=f32
    )


def analyse_kernel(v_ref, ex_ref, ey_ref, o_ref):
    count = v_ref.shape[0]
    ex2, eyt = ex_ref[...], ey_ref[...]
    out = slab_modes(lambda s: v_ref[s], count, ex2, eyt)
    o_ref[...] = out.reshape(o_ref.shape)


def analyse_slabs(volume, ex2, eyt):
    slabs, size_x, size_y = volume.shape
    modes = eyt.shape[1]
    block = 16
    return pl.pallas_call(
        analyse_kernel,
        grid=(slabs // block,),
        in_specs=[
            pl.BlockSpec((block, size_x, size_y), lambda g: (g, 0, 0)),
            pl.BlockSpec(ex2.shape, lambda g: (0, 0)),
            pl.BlockSpec(eyt.shape, lambda g: (0, 0)),
        ],
        out_specs=pl.BlockSpec((block, modes, modes), lambda g: (g, 0, 0)),
        out_shape=jax.ShapeDtypeStruct((slabs, modes, modes), f32),
        compiler_params=params("arbitrary"),
        name="analyse",
    )(volume, ex2, eyt)


def chunk_specs(height, rows, size_x, size_y):
    return [
        pl.BlockSpec((height, size_y), lambda g: (0, (g * rows + size_x - 1) % size_x)),
        pl.BlockSpec((height, rows * size_y), lambda g: (0, g)),
        pl.BlockSpec((height, size_y), lambda g: (0, (g * rows + rows) % size_x)),
    ]


def conv_kernel(rows, size_y, low_ref, mid_ref, high_ref, w_ref, o_ref):
    span = rows * size_y
    block = jnp.concatenate([low_ref[...], mid_ref[...], high_ref[...]], axis=1)
    stacked = jnp.concatenate(
        [block[:, b * size_y : b * size_y + span] for b in range(3)], axis=0
    )
    total = jnp.dot(w_ref[...], stacked, preferred_element_type=f32)
    count = total.shape[0] // 3
    flat = o_ref.reshape(count * rows, size_y)
    for r in range(rows):
        piece = total[:, r * size_y : (r + 1) * size_y]
        value = (
            pltpu.roll(piece[:count], 1, 1)
            + piece[count : 2 * count]
            + pltpu.roll(piece[2 * count :], size_y - 1, 1)
        )
        flat[pl.ds(r, count, stride=rows), :] = value


def forward_conv(flat, weights, size_x, size_y):
    count = weights.shape[0] // 3
    rows = 8
    return pl.pallas_call(
        partial(conv_kernel, rows, size_y),
        grid=(size_x // rows,),
        in_specs=chunk_specs(flat.shape[0], rows, size_x, size_y)
        + [pl.BlockSpec(weights.shape, lambda g: (0, 0))],
        out_specs=pl.BlockSpec((count, rows, size_y), lambda g: (0, g, 0)),
        out_shape=jax.ShapeDtypeStruct((count, size_x, size_y), f32),
        compiler_params=params("arbitrary"),
        name="forward_conv",
    )(flat, flat, flat, weights)


def planar(spectrum, ext, ey):
    along_x = jnp.dot(ext, spectrum, precision=highest, preferred_element_type=f32)
    return jnp.dot(along_x, ey, precision=highest, preferred_element_type=f32)


def gelu_kernel(c_ref, lo_ref, hi_ref, s_ref, g_ref, ext_ref, ey_ref, ex2_ref, eyt_ref,
                out_ref, gp_ref, m_ref):
    plane = pl.program_id(0)
    last = pl.num_programs(0) - 1
    count = c_ref.shape[1]
    keep_lo = jnp.where(plane == 0, 1.0, 0.0).astype(f32)
    keep_hi = jnp.where(plane == last, 1.0, 0.0).astype(f32)
    ext, ey = ext_ref[...], ey_ref[...]
    k0 = math.sqrt(2.0 / math.pi)
    k1 = 0.044715
    for o in range(count):
        v = c_ref[0, o] + lo_ref[o].astype(f32) * keep_lo + hi_ref[o].astype(f32) * keep_hi
        v = v + planar(s_ref[0, o], ext, ey)
        v2 = v * v
        t = jnp.tanh(k0 * v * (1.0 + k1 * v2))
        half = 0.5 * (1.0 + t)
        out_ref[o, 0] = (v * half).astype(bf16)
        slope = half + (0.5 * k0) * v * (1.0 - t * t) * (1.0 + (3.0 * k1) * v2)
        gp_ref[0, o] = (g_ref[o, 0].astype(f32) * slope).astype(bf16)
    modes = slab_modes(lambda o: gp_ref[0, o], count, ex2_ref[...], eyt_ref[...])
    m_ref[...] = modes.reshape(m_ref.shape)


def gelu_stage(conv, low, high, slabs, grad_out, tables):
    ext, ey, ex2, eyt = tables
    share, planes, size_x, size_y = grad_out.shape
    modes = ey.shape[0]
    block = 8
    field = pl.BlockSpec((block, 1, size_x, size_y), lambda z, g: (g, z, 0, 0))
    rim = pl.BlockSpec((block, size_x, size_y), lambda z, g: (g, 0, 0))
    whole = lambda t: pl.BlockSpec(t.shape, lambda z, g: (0, 0))
    return pl.pallas_call(
        gelu_kernel,
        grid=(planes, share // block),
        in_specs=[
            pl.BlockSpec((1, block, size_x, size_y), lambda z, g: (z + 1, g, 0, 0)),
            rim,
            rim,
            pl.BlockSpec((1, block, modes, modes), lambda z, g: (z, g, 0, 0)),
            field,
            whole(ext),
            whole(ey),
            whole(ex2),
            whole(eyt),
        ],
        out_specs=[
            field,
            pl.BlockSpec((1, block, size_x, size_y), lambda z, g: (z, g, 0, 0)),
            pl.BlockSpec((1, block, modes, modes), lambda z, g: (z, g, 0, 0)),
        ],
        out_shape=[
            jax.ShapeDtypeStruct(grad_out.shape, bf16),
            jax.ShapeDtypeStruct((planes, share, size_x, size_y), bf16),
            jax.ShapeDtypeStruct((planes, share, modes, modes), f32),
        ],
        compiler_params=params("arbitrary", "arbitrary"),
        name="gelu_stage",
    )(conv, low, high, slabs, grad_out, ext, ey, ex2, eyt)


def back_kernel(rows, size_y, planes, low_ref, mid_ref, high_ref, f_ref, w_ref, c_ref, t_ref,
                acc_ref):
    step = pl.program_id(0)
    height = mid_ref.shape[0]
    depth = f_ref.shape[0]
    span = rows * size_y
    pieces = [low_ref[...]]
    pieces += [mid_ref[:, r * size_y : (r + 1) * size_y] for r in range(rows)]
    pieces.append(high_ref[...])
    wide = [piece.astype(f32) for piece in pieces]
    columns = [
        [pltpu.roll(piece, size_y - 1, 1).astype(bf16) for piece in wide],
        pieces,
        [pltpu.roll(piece, 1, 1).astype(bf16) for piece in wide],
    ]
    columns = [jnp.concatenate(column, axis=1) for column in columns]
    stacked = jnp.concatenate(
        [
            column[:, (2 - b) * size_y : (2 - b) * size_y + span]
            for b in range(3)
            for column in columns
        ],
        axis=0,
    )
    c_ref[...] = jnp.dot(w_ref[...], stacked, preferred_element_type=f32).astype(bf16)
    product = lax.dot_general(
        stacked, f_ref[...], (((1,), (1,)), ((), ())), preferred_element_type=f32
    )

    @pl.when(step == 0)
    def _():
        acc_ref[...] = product

    @pl.when(step > 0)
    def _():
        acc_ref[...] += product

    @pl.when(step == pl.num_programs(0) - 1)
    def _():
        share = height // (planes + 2)
        channels = depth // planes
        for a in range(3):
            for k in range(9):
                total = None
                for z in range(planes):
                    first = k * height + (z - a + 2) * share
                    term = acc_ref[first : first + share, :]
                    if z:
                        term = pltpu.roll(term, depth - z * channels, 1)
                    total = term if total is None else total + term
                out = (9 * a + k) * share
                t_ref[out : out + share, :] = total[:, :channels]


def backward_convs(grads, flat, weights, planes, size_x, size_y):
    height = grads.shape[0]
    depth = flat.shape[0]
    rows = 8
    span = rows * size_y
    taps = (27 * height // (planes + 2), depth // planes)
    return pl.pallas_call(
        partial(back_kernel, rows, size_y, planes),
        grid=(size_x // rows,),
        in_specs=chunk_specs(height, rows, size_x, size_y)
        + [
            pl.BlockSpec((depth, span), lambda g: (0, g)),
            pl.BlockSpec(weights.shape, lambda g: (0, 0)),
        ],
        out_specs=[
            pl.BlockSpec((depth, span), lambda g: (0, g)),
            pl.BlockSpec(taps, lambda g: (0, 0)),
        ],
        out_shape=[
            jax.ShapeDtypeStruct((depth, size_x * size_y), bf16),
            jax.ShapeDtypeStruct(taps, f32),
        ],
        scratch_shapes=[pltpu.VMEM((9 * height, depth), f32)],
        compiler_params=params("arbitrary"),
        name="backward_convs",
    )(grads, grads, grads, flat, weights)


def final_kernel(a_ref, b_ref, s_ref, ext_ref, ey_ref, o_ref):
    ext, ey = ext_ref[...], ey_ref[...]
    for i in range(a_ref.shape[1]):
        total = a_ref[0, i].astype(f32) + b_ref[0, i].astype(f32)
        o_ref[i, 0] = (total + planar(s_ref[0, i], ext, ey)).astype(bf16)


def final_stage(own, other, slabs, tables):
    ext, ey = tables[:2]
    planes, share, size_x, size_y = own.shape
    modes = ey.shape[0]
    block = 8
    field = pl.BlockSpec((1, block, size_x, size_y), lambda z, g: (z, g, 0, 0))
    return pl.pallas_call(
        final_kernel,
        grid=(planes, share // block),
        in_specs=[
            field,
            field,
            pl.BlockSpec((1, block, modes, modes), lambda z, g: (z, g, 0, 0)),
            pl.BlockSpec(ext.shape, lambda z, g: (0, 0)),
            pl.BlockSpec(ey.shape, lambda z, g: (0, 0)),
        ],
        out_specs=pl.BlockSpec((block, 1, size_x, size_y), lambda z, g: (g, z, 0, 0)),
        out_shape=jax.ShapeDtypeStruct((share, planes, size_x, size_y), bf16),
        compiler_params=params("arbitrary", "arbitrary"),
        name="final_stage",
    )(own, other, slabs, ext, ey)


def to_modes(planes, table_z):
    gathered = lax.all_to_all(planes, "gz", split_axis=2, concat_axis=1, tiled=True)
    return jnp.einsum("jz,czm->cjm", table_z, gathered, precision=highest)


def to_slabs(spectrum, table_z):
    columns = jnp.einsum("jz,cjm->czm", table_z, spectrum, precision=highest)
    return lax.all_to_all(columns, "gz", split_axis=1, concat_axis=2, tiled=True)


def plane_slabs(spectrum, table_z, planes):
    slabs = to_slabs(spectrum, table_z)
    modes = table_z.shape[0]
    return jnp.transpose(slabs.reshape(-1, planes, modes, modes), (1, 0, 2, 3))


def halve(block, bit):
    count = lax.axis_size("col")
    side = (lax.axis_index("col") // bit) % 2
    pairs = [(i, i ^ bit) for i in range(count)]
    mine = lax.dynamic_index_in_dim(block, side, 2, keepdims=False)
    other = lax.dynamic_index_in_dim(block, 1 - side, 2, keepdims=False)
    return mine, lax.ppermute(other, "col", pairs)


def sum_over_slabs(terms):
    groups = lax.axis_size("gz")
    pieces = lax.all_to_all(terms.reshape(groups, -1), "gz", split_axis=0, concat_axis=0, tiled=True)
    total = lax.all_gather(jnp.sum(pieces, axis=0), "gz", axis=0, tiled=True)
    return total.reshape(terms.shape)


def local(features, grad_out, conv_weight, spectral_weight):
    channels, planes, size_x, size_y = features.shape
    share = conv_weight.shape[0]
    modes = spectral_weight.shape[2]
    groups = lax.axis_size("gz")
    parts = lax.axis_size("col")
    table_x = basis(size_x, modes)
    table_y = basis(size_y, modes)
    table_z = basis(planes * groups, modes)
    ex2 = np.concatenate(split_table(table_x), axis=0)
    eyt = np.ascontiguousarray(table_y.astype(bf16).T)
    tables = tuple(
        jnp.asarray(t) for t in (np.ascontiguousarray(table_x.T), table_y, ex2, eyt)
    )
    table_z = jnp.asarray(table_z)
    up, down = neighbours("gz")

    taps = conv_weight.reshape(share, channels, 3, 9)[:, :, ::-1]
    taps = jnp.transpose(taps, (1, 3, 2, 0)).reshape(channels, 9, 3 * share)
    w_back = jnp.stack(
        [
            jnp.pad(taps, ((0, 0), (0, 0), (z * share, (planes - 1 - z) * share)))
            for z in range(planes)
        ]
    ).reshape(planes * channels, 9 * share * (planes + 2))
    thirds = w_back.shape[1] // 3
    w_forward = jnp.concatenate(
        [w_back[:, b * thirds : (b + 1) * thirds].T for b in range(3)], axis=1
    )

    first_channel = lax.axis_index("col") * share
    own = lax.dynamic_slice_in_dim(features, first_channel, share, 0)
    planar_modes = analyse_slabs(own.reshape(share * planes, size_x, size_y), *tables[2:])
    spectrum = to_modes(planar_modes.reshape(share, planes, modes * modes), table_z)
    spectrum_all = lax.all_gather(spectrum, "col", axis=0, tiled=True)

    flat = jnp.transpose(features, (1, 0, 2, 3)).reshape(planes * channels, size_x * size_y)
    conv = forward_conv(flat, w_forward, size_x, size_y)
    conv = conv.reshape(planes + 2, share, size_x, size_y)
    low = lax.ppermute(conv[planes + 1].astype(bf16), "gz", up)
    high = lax.ppermute(conv[0].astype(bf16), "gz", down)

    weights32 = spectral_weight.astype(f32)
    mixed = jnp.sum(weights32 * spectrum_all[:, None], axis=0)
    slabs = plane_slabs(mixed, table_z, planes)
    layer_out, grad_pre, grad_planar = gelu_stage(conv, low, high, slabs, grad_out, tables)

    before = lax.ppermute(grad_pre[planes - 1 :], "gz", up)
    after = lax.ppermute(grad_pre[:1], "gz", down)
    grad_planar = jnp.transpose(grad_planar, (1, 0, 2, 3)).reshape(share, planes, modes * modes)
    grad_modes = to_modes(grad_planar, table_z)

    rimmed = jnp.concatenate([before, grad_pre, after], axis=0)
    rimmed = rimmed.reshape((planes + 2) * share, size_x * size_y)
    contributions, products = backward_convs(rimmed, flat, w_back, planes, size_x, size_y)
    block = contributions.reshape(planes, parts, share, size_x * size_y)
    bit = 1
    received = None
    while bit < parts:
        if received is not None:
            block = (block.astype(f32) + received.astype(f32)).astype(bf16)
        paired = block.reshape(planes, block.shape[1] // 2, 2, *block.shape[2:])
        block, received = halve(paired, bit)
        bit *= 2
    shape = (planes, share, size_x, size_y)
    block, received = block.reshape(shape), received.reshape(shape)

    scaling = 1.0 / math.sqrt(size_x * size_y * planes * groups)
    grad_conv = sum_over_slabs(products) * scaling
    grad_conv = jnp.transpose(grad_conv.reshape(27, share, channels), (1, 2, 0))

    back_terms = jnp.sum(weights32 * grad_modes[None], axis=1)
    back_modes = lax.psum_scatter(
        back_terms.astype(bf16), "col", scatter_dimension=0, tiled=True
    ).astype(f32)
    back_slabs = plane_slabs(back_modes, table_z, planes)
    grad_input = final_stage(block, received, back_slabs, tables)
    grad_spectral = spectrum_all[:, None] * grad_modes[None]
    return (layer_out, grad_input, grad_conv, grad_spectral)


def solution(mesh):
    return jax.shard_map(
        local,
        mesh=mesh,
        in_specs=(
            P(None, "gz", None, None),
            P("col", "gz", None, None),
            P("col", None, None),
            P(None, "col", None, "gz"),
        ),
        out_specs=(
            P("col", "gz", None, None),
            P("col", "gz", None, None),
            P("col", None, None),
            P(None, "col", None, "gz"),
        ),
        check_vma=False,
    )
```

```python
from functools import partial
import math

import jax
import jax.numpy as jnp
import numpy as np
from jax import lax
from jax.experimental import pallas as pl
from jax.experimental.pallas import tpu as pltpu
from jax.sharding import PartitionSpec as P

highest = lax.Precision.HIGHEST
f32 = jnp.float32
bf16 = jnp.bfloat16


def basis(length, mode_count):
    indices = np.arange(mode_count)
    middle = mode_count // 2
    cosine_rows = indices <= middle
    frequency = np.where(cosine_rows, indices, indices - middle)
    residue = frequency[:, None] * np.arange(length)[None, :] % length
    radians = residue * (2.0 * math.pi / length)
    tables = np.where(cosine_rows[:, None], np.cos(radians), np.sin(radians))
    return (tables * math.sqrt(2.0 / length)).astype(np.float32)


def split_table(table):
    high = table.astype(bf16)
    return high, (table - high.astype(np.float32)).astype(bf16)


def neighbours(axis):
    count = lax.axis_size(axis)
    up = [(i, (i + 1) % count) for i in range(count)]
    down = [((i + 1) % count, i) for i in range(count)]
    return up, down


def params(*semantics):
    return pltpu.CompilerParams(
        dimension_semantics=semantics, vmem_limit_bytes=48 * 1024 * 1024
    )


def slab_modes(slab_of, count, ex2, eyt):
    modes = ex2.shape[0] // 2
    parts = []
    for s in range(count):
        both = jnp.dot(ex2, slab_of(s), preferred_element_type=f32)
        parts.append(both[:modes] + both[modes:])
    along_x = jnp.concatenate(parts, axis=0)
    high = along_x.astype(bf16)
    low = (along_x - high.astype(f32)).astype(bf16)
    return jnp.dot(high, eyt, preferred_element_type=f32) + jnp.dot(
        low, eyt, preferred_element_type=f32
    )


def analyse_kernel(v_ref, ex_ref, ey_ref, o_ref):
    count = v_ref.shape[0]
    ex2, eyt = ex_ref[...], ey_ref[...]
    out = slab_modes(lambda s: v_ref[s], count, ex2, eyt)
    o_ref[...] = out.reshape(o_ref.shape)


def analyse_slabs(volume, ex2, eyt):
    slabs, size_x, size_y = volume.shape
    modes = eyt.shape[1]
    block = 16
    return pl.pallas_call(
        analyse_kernel,
        grid=(slabs // block,),
        in_specs=[
            pl.BlockSpec((block, size_x, size_y), lambda g: (g, 0, 0)),
            pl.BlockSpec(ex2.shape, lambda g: (0, 0)),
            pl.BlockSpec(eyt.shape, lambda g: (0, 0)),
        ],
        out_specs=pl.BlockSpec((block, modes, modes), lambda g: (g, 0, 0)),
        out_shape=jax.ShapeDtypeStruct((slabs, modes, modes), f32),
        compiler_params=params("arbitrary"),
        name="analyse",
    )(volume, ex2, eyt)


def chunk_specs(height, rows, size_x, size_y):
    return [
        pl.BlockSpec((height, size_y), lambda g: (0, (g * rows + size_x - 1) % size_x)),
        pl.BlockSpec((height, rows * size_y), lambda g: (0, g)),
        pl.BlockSpec((height, size_y), lambda g: (0, (g * rows + rows) % size_x)),
    ]


def conv_kernel(rows, size_y, low_ref, mid_ref, high_ref, w_ref, o_ref):
    span = rows * size_y
    block = jnp.concatenate([low_ref[...], mid_ref[...], high_ref[...]], axis=1)
    stacked = jnp.concatenate(
        [block[:, b * size_y : b * size_y + span] for b in range(3)], axis=0
    )
    total = jnp.dot(w_ref[...], stacked, preferred_element_type=f32)
    count = total.shape[0] // 3
    flat = o_ref.reshape(count * rows, size_y)
    for r in range(rows):
        piece = total[:, r * size_y : (r + 1) * size_y]
        value = (
            pltpu.roll(piece[:count], 1, 1)
            + piece[count : 2 * count]
            + pltpu.roll(piece[2 * count :], size_y - 1, 1)
        )
        flat[pl.ds(r, count, stride=rows), :] = value


def forward_conv(flat, weights, size_x, size_y):
    count = weights.shape[0] // 3
    rows = 8
    return pl.pallas_call(
        partial(conv_kernel, rows, size_y),
        grid=(size_x // rows,),
        in_specs=chunk_specs(flat.shape[0], rows, size_x, size_y)
        + [pl.BlockSpec(weights.shape, lambda g: (0, 0))],
        out_specs=pl.BlockSpec((count, rows, size_y), lambda g: (0, g, 0)),
        out_shape=jax.ShapeDtypeStruct((count, size_x, size_y), f32),
        compiler_params=params("arbitrary"),
        name="forward_conv",
    )(flat, flat, flat, weights)


def planar(spectrum, ext, ey):
    along_x = jnp.dot(ext, spectrum, precision=highest, preferred_element_type=f32)
    return jnp.dot(along_x, ey, precision=highest, preferred_element_type=f32)


def gelu_kernel(c_ref, lo_ref, hi_ref, s_ref, g_ref, ext_ref, ey_ref, ex2_ref, eyt_ref,
                out_ref, gp_ref, m_ref):
    plane = pl.program_id(0)
    last = pl.num_programs(0) - 1
    count = c_ref.shape[1]
    keep_lo = jnp.where(plane == 0, 1.0, 0.0).astype(f32)
    keep_hi = jnp.where(plane == last, 1.0, 0.0).astype(f32)
    ext, ey = ext_ref[...], ey_ref[...]
    k0 = math.sqrt(2.0 / math.pi)
    k1 = 0.044715
    for o in range(count):
        v = c_ref[0, o] + lo_ref[o].astype(f32) * keep_lo + hi_ref[o].astype(f32) * keep_hi
        v = v + planar(s_ref[0, o], ext, ey)
        v2 = v * v
        t = jnp.tanh(k0 * v * (1.0 + k1 * v2))
        half = 0.5 * (1.0 + t)
        out_ref[o, 0] = (v * half).astype(bf16)
        slope = half + (0.5 * k0) * v * (1.0 - t * t) * (1.0 + (3.0 * k1) * v2)
        gp_ref[0, o] = (g_ref[o, 0].astype(f32) * slope).astype(bf16)
    modes = slab_modes(lambda o: gp_ref[0, o], count, ex2_ref[...], eyt_ref[...])
    m_ref[...] = modes.reshape(m_ref.shape)


def gelu_stage(conv, low, high, slabs, grad_out, tables):
    ext, ey, ex2, eyt = tables
    share, planes, size_x, size_y = grad_out.shape
    modes = ey.shape[0]
    block = 8
    field = pl.BlockSpec((block, 1, size_x, size_y), lambda z, g: (g, z, 0, 0))
    rim = pl.BlockSpec((block, size_x, size_y), lambda z, g: (g, 0, 0))
    whole = lambda t: pl.BlockSpec(t.shape, lambda z, g: (0, 0))
    return pl.pallas_call(
        gelu_kernel,
        grid=(planes, share // block),
        in_specs=[
            pl.BlockSpec((1, block, size_x, size_y), lambda z, g: (z + 1, g, 0, 0)),
            rim,
            rim,
            pl.BlockSpec((1, block, modes, modes), lambda z, g: (z, g, 0, 0)),
            field,
            whole(ext),
            whole(ey),
            whole(ex2),
            whole(eyt),
        ],
        out_specs=[
            field,
            pl.BlockSpec((1, block, size_x, size_y), lambda z, g: (z, g, 0, 0)),
            pl.BlockSpec((1, block, modes, modes), lambda z, g: (z, g, 0, 0)),
        ],
        out_shape=[
            jax.ShapeDtypeStruct(grad_out.shape, bf16),
            jax.ShapeDtypeStruct((planes, share, size_x, size_y), bf16),
            jax.ShapeDtypeStruct((planes, share, modes, modes), f32),
        ],
        compiler_params=params("arbitrary", "arbitrary"),
        name="gelu_stage",
    )(conv, low, high, slabs, grad_out, ext, ey, ex2, eyt)


def back_kernel(rows, size_y, planes, low_ref, mid_ref, high_ref, f_ref, w_ref, c_ref, t_ref,
                acc_ref):
    step = pl.program_id(0)
    height = mid_ref.shape[0]
    depth = f_ref.shape[0]
    span = rows * size_y
    pieces = [low_ref[...]]
    pieces += [mid_ref[:, r * size_y : (r + 1) * size_y] for r in range(rows)]
    pieces.append(high_ref[...])
    wide = [piece.astype(f32) for piece in pieces]
    columns = [
        [pltpu.roll(piece, size_y - 1, 1).astype(bf16) for piece in wide],
        pieces,
        [pltpu.roll(piece, 1, 1).astype(bf16) for piece in wide],
    ]
    columns = [jnp.concatenate(column, axis=1) for column in columns]
    stacked = jnp.concatenate(
        [
            column[:, (2 - b) * size_y : (2 - b) * size_y + span]
            for b in range(3)
            for column in columns
        ],
        axis=0,
    )
    c_ref[...] = jnp.dot(w_ref[...], stacked, preferred_element_type=f32).astype(bf16)
    product = lax.dot_general(
        stacked, f_ref[...], (((1,), (1,)), ((), ())), preferred_element_type=f32
    )

    @pl.when(step == 0)
    def _():
        acc_ref[...] = product

    @pl.when(step > 0)
    def _():
        acc_ref[...] += product

    @pl.when(step == pl.num_programs(0) - 1)
    def _():
        share = height // (planes + 2)
        channels = depth // planes
        for a in range(3):
            for k in range(9):
                total = None
                for z in range(planes):
                    first = k * height + (z - a + 2) * share
                    term = acc_ref[first : first + share, :]
                    if z:
                        term = pltpu.roll(term, depth - z * channels, 1)
                    total = term if total is None else total + term
                out = (9 * a + k) * share
                t_ref[out : out + share, :] = total[:, :channels]


def backward_convs(grads, flat, weights, planes, size_x, size_y):
    height = grads.shape[0]
    depth = flat.shape[0]
    rows = 8
    span = rows * size_y
    taps = (27 * height // (planes + 2), depth // planes)
    return pl.pallas_call(
        partial(back_kernel, rows, size_y, planes),
        grid=(size_x // rows,),
        in_specs=chunk_specs(height, rows, size_x, size_y)
        + [
            pl.BlockSpec((depth, span), lambda g: (0, g)),
            pl.BlockSpec(weights.shape, lambda g: (0, 0)),
        ],
        out_specs=[
            pl.BlockSpec((depth, span), lambda g: (0, g)),
            pl.BlockSpec(taps, lambda g: (0, 0)),
        ],
        out_shape=[
            jax.ShapeDtypeStruct((depth, size_x * size_y), bf16),
            jax.ShapeDtypeStruct(taps, f32),
        ],
        scratch_shapes=[pltpu.VMEM((9 * height, depth), f32)],
        compiler_params=params("arbitrary"),
        name="backward_convs",
    )(grads, grads, grads, flat, weights)


def final_kernel(a_ref, b_ref, s_ref, ext_ref, ey_ref, o_ref):
    ext, ey = ext_ref[...], ey_ref[...]
    for i in range(a_ref.shape[1]):
        total = a_ref[0, i].astype(f32) + b_ref[0, i].astype(f32)
        o_ref[i, 0] = (total + planar(s_ref[0, i], ext, ey)).astype(bf16)


def final_stage(own, other, slabs, tables):
    ext, ey = tables[:2]
    planes, share, size_x, size_y = own.shape
    modes = ey.shape[0]
    block = 8
    field = pl.BlockSpec((1, block, size_x, size_y), lambda z, g: (z, g, 0, 0))
    return pl.pallas_call(
        final_kernel,
        grid=(planes, share // block),
        in_specs=[
            field,
            field,
            pl.BlockSpec((1, block, modes, modes), lambda z, g: (z, g, 0, 0)),
            pl.BlockSpec(ext.shape, lambda z, g: (0, 0)),
            pl.BlockSpec(ey.shape, lambda z, g: (0, 0)),
        ],
        out_specs=pl.BlockSpec((block, 1, size_x, size_y), lambda z, g: (g, z, 0, 0)),
        out_shape=jax.ShapeDtypeStruct((share, planes, size_x, size_y), bf16),
        compiler_params=params("arbitrary", "arbitrary"),
        name="final_stage",
    )(own, other, slabs, ext, ey)


def to_modes(planes, table_z):
    gathered = lax.all_to_all(planes, "gz", split_axis=2, concat_axis=1, tiled=True)
    return jnp.einsum("jz,czm->cjm", table_z, gathered, precision=highest)


def to_slabs(spectrum, table_z):
    columns = jnp.einsum("jz,cjm->czm", table_z, spectrum, precision=highest)
    return lax.all_to_all(columns, "gz", split_axis=1, concat_axis=2, tiled=True)


def plane_slabs(spectrum, table_z, planes):
    slabs = to_slabs(spectrum, table_z)
    modes = table_z.shape[0]
    return jnp.transpose(slabs.reshape(-1, planes, modes, modes), (1, 0, 2, 3))


def halve(block, bit):
    count = lax.axis_size("col")
    side = (lax.axis_index("col") // bit) % 2
    pairs = [(i, i ^ bit) for i in range(count)]
    mine = lax.dynamic_index_in_dim(block, side, 2, keepdims=False)
    other = lax.dynamic_index_in_dim(block, 1 - side, 2, keepdims=False)
    return mine, lax.ppermute(other, "col", pairs)


def sum_over_slabs(terms):
    groups = lax.axis_size("gz")
    pieces = lax.all_to_all(terms.reshape(groups, -1), "gz", split_axis=0, concat_axis=0, tiled=True)
    total = jnp.broadcast_to(jnp.sum(pieces, axis=0)[None], pieces.shape)
    total = lax.all_to_all(total, "gz", split_axis=0, concat_axis=0, tiled=True)
    return total.reshape(terms.shape)


def local(features, grad_out, conv_weight, spectral_weight):
    channels, planes, size_x, size_y = features.shape
    share = conv_weight.shape[0]
    modes = spectral_weight.shape[2]
    groups = lax.axis_size("gz")
    parts = lax.axis_size("col")
    table_x = basis(size_x, modes)
    table_y = basis(size_y, modes)
    table_z = basis(planes * groups, modes)
    ex2 = np.concatenate(split_table(table_x), axis=0)
    eyt = np.ascontiguousarray(table_y.astype(bf16).T)
    tables = tuple(
        jnp.asarray(t) for t in (np.ascontiguousarray(table_x.T), table_y, ex2, eyt)
    )
    table_z = jnp.asarray(table_z)
    up, down = neighbours("gz")

    taps = conv_weight.reshape(share, channels, 3, 9)[:, :, ::-1]
    taps = jnp.transpose(taps, (1, 3, 2, 0)).reshape(channels, 9, 3 * share)
    w_back = jnp.stack(
        [
            jnp.pad(taps, ((0, 0), (0, 0), (z * share, (planes - 1 - z) * share)))
            for z in range(planes)
        ]
    ).reshape(planes * channels, 9 * share * (planes + 2))
    thirds = w_back.shape[1] // 3
    w_forward = jnp.concatenate(
        [w_back[:, b * thirds : (b + 1) * thirds].T for b in range(3)], axis=1
    )

    first_channel = lax.axis_index("col") * share
    own = lax.dynamic_slice_in_dim(features, first_channel, share, 0)
    planar_modes = analyse_slabs(own.reshape(share * planes, size_x, size_y), *tables[2:])
    spectrum = to_modes(planar_modes.reshape(share, planes, modes * modes), table_z)
    spectrum_all = lax.all_gather(spectrum, "col", axis=0, tiled=True)

    flat = jnp.transpose(features, (1, 0, 2, 3)).reshape(planes * channels, size_x * size_y)
    conv = forward_conv(flat, w_forward, size_x, size_y)
    conv = conv.reshape(planes + 2, share, size_x, size_y)
    low = lax.ppermute(conv[planes + 1].astype(bf16), "gz", up)
    high = lax.ppermute(conv[0].astype(bf16), "gz", down)

    weights32 = spectral_weight.astype(f32)
    mixed = jnp.sum(weights32 * spectrum_all[:, None], axis=0)
    slabs = plane_slabs(mixed, table_z, planes)
    layer_out, grad_pre, grad_planar = gelu_stage(conv, low, high, slabs, grad_out, tables)

    before = lax.ppermute(grad_pre[planes - 1 :], "gz", up)
    after = lax.ppermute(grad_pre[:1], "gz", down)
    grad_planar = jnp.transpose(grad_planar, (1, 0, 2, 3)).reshape(share, planes, modes * modes)
    grad_modes = to_modes(grad_planar, table_z)

    back_terms = jnp.sum(weights32 * grad_modes[None], axis=1).astype(bf16)
    quarters = lax.all_to_all(back_terms, "col", split_axis=0, concat_axis=0, tiled=True)
    quarters = quarters.reshape(parts, share, *back_terms.shape[1:])
    back_modes = jnp.sum(quarters.astype(f32), axis=0)
    back_slabs = plane_slabs(back_modes, table_z, planes)
    before, after, back_slabs = lax.optimization_barrier((before, after, back_slabs))

    rimmed = jnp.concatenate([before, grad_pre, after], axis=0)
    rimmed = rimmed.reshape((planes + 2) * share, size_x * size_y)
    contributions, products = backward_convs(rimmed, flat, w_back, planes, size_x, size_y)
    block = contributions.reshape(planes, parts, share, size_x * size_y)
    bit = 1
    received = None
    while bit < parts:
        if received is not None:
            block = (block.astype(f32) + received.astype(f32)).astype(bf16)
        paired = block.reshape(planes, block.shape[1] // 2, 2, *block.shape[2:])
        block, received = halve(paired, bit)
        bit *= 2
    shape = (planes, share, size_x, size_y)
    block, received = block.reshape(shape), received.reshape(shape)

    scaling = 1.0 / math.sqrt(size_x * size_y * planes * groups)
    grad_conv = sum_over_slabs(products) * scaling
    grad_conv = jnp.transpose(grad_conv.reshape(27, share, channels), (1, 2, 0))

    grad_input = final_stage(block, received, back_slabs, tables)
    grad_spectral = spectrum_all[:, None] * grad_modes[None]
    return (layer_out, grad_input, grad_conv, grad_spectral)


def solution(mesh):
    return jax.shard_map(
        local,
        mesh=mesh,
        in_specs=(
            P(None, "gz", None, None),
            P("col", "gz", None, None),
            P("col", None, None),
            P(None, "col", None, "gz"),
        ),
        out_specs=(
            P("col", "gz", None, None),
            P("col", "gz", None, None),
            P("col", None, None),
            P(None, "col", None, "gz"),
        ),
        check_vma=False,
    )
```
